128 devices in a mesh: rep: 1, r: 4 (over x), s: 32 (over y, z, core).
Axes of the slice: x: 4, y: 4, z: 4, core: 2. Of those that a mesh axis runs over, the one named last changes fastest.
Arguments:
- x: bfloat16 [128, 2048, 1280], P(('rep', 'r', 's'))
- dy: bfloat16 [128, 2048, 1280], P(('rep', 'r', 's'))
- w_gate: bfloat16 [2, 1280, 4480], P(None, 's')
- w_up: bfloat16 [2, 1280, 4480], P(None, 's')
- w_down: bfloat16 [2, 4480, 1280], P(None, 's')
Outputs:
- output 1: bfloat16 [128, 2048, 1280], P(('rep', 'r', 's'))
- output 2: bfloat16 [2, 1280, 4480], P('rep', 's')
- output 3: bfloat16 [2, 1280, 4480], P('rep', 's')
- output 4: bfloat16 [2, 4480, 1280], P('rep', 's')
All inputs are finite; a program needn't handle non-finite values.
Results may differ from the reference program's by a relative error of at most 0.018.
Values are sent between devices in bfloat16 or wider.
A program may use at most 1.5 GiB of HBM per device.

```python
import jax
import jax.numpy as jnp
from jax import lax

SEQUENCES = 128
TOKENS = 2048
D = 1280
FF = 4480
LAYERS = 2
NAMES = ("w_gate", "w_up", "w_down")
SHAPES = {"w_gate": (LAYERS, D, FF), "w_up": (LAYERS, D, FF), "w_down": (LAYERS, FF, D)}


def bump(key, n, height):
    away = (jnp.arange(n, dtype=jnp.int32) - jax.random.randint(key, (), 0, n, jnp.int32)) % n
    return jnp.where(away < n // 8, height, 1.0)


def together(key, own, strength):
    shared = jax.random.normal(key, own.shape[1:], jnp.float32)
    return (own + strength * shared) * lax.rsqrt(1 + strength * strength)


def setup_inputs(seed: int = 0, part: int = 0) -> dict:
    kx, kdy, ka, kb, kz, kf, kh, kl, *kw = jax.random.split(jax.random.key(seed), 8 + len(NAMES))
    kx, kdy, ka, kb = (jax.random.fold_in(k, part) for k in (kx, kdy, ka, kb))
    shape = (SEQUENCES, TOKENS, D)
    much_x, much_dy = jax.random.uniform(kz, (2,), jnp.float32, 0.0, 1.0)
    layers = 2.0 ** jax.random.uniform(kl, (LAYERS, 1, 1), jnp.float32, -1.0, 1.0)
    x = together(ka, jax.random.normal(kx, shape, jnp.float32), much_x) * bump(kf, D, 4.0)
    dy = together(kb, jax.random.normal(kdy, shape, jnp.float32), much_dy)
    drawn = {"x": x.astype(jnp.bfloat16), "dy": (dy * (SEQUENCES * TOKENS) ** -0.5).astype(jnp.bfloat16)}
    for key, name in zip(kw, NAMES, strict=True):
        w = jax.random.normal(key, SHAPES[name], jnp.float32) * SHAPES[name][1] ** -0.5
        drawn[name] = (w * {"w_gate": 1.0, "w_up": bump(kh, FF, 4.0), "w_down": layers}[name]).astype(jnp.bfloat16)
    return drawn


def matmul(a, w):
    return jnp.dot(a, w, preferred_element_type=jnp.float32).astype(jnp.bfloat16)


def normed(h):
    wide = h.astype(jnp.float32)
    scale = lax.rsqrt(jnp.mean(wide**2, -1, keepdims=True) + 1e-6)
    return (wide * scale).astype(jnp.bfloat16)


def layer(h, w):
    a = normed(h)
    gate = jnp.dot(a, w["w_gate"], preferred_element_type=jnp.float32)
    up = jnp.dot(a, w["w_up"], preferred_element_type=jnp.float32)
    return h + matmul((jax.nn.silu(gate) * up).astype(jnp.bfloat16), w["w_down"])


def stack(weights, h):
    return lax.scan(lambda h, w: (layer(h, w), None), h, weights)[0]


def reference(x, dy, w_gate, w_up, w_down):
    weights = dict(zip(NAMES, (w_gate, w_up, w_down), strict=True))

    def take(so_far, sequence):
        h, by_y = sequence
        _, back = jax.vjp(stack, weights, h)
        by_weights, by_h = back(by_y)
        return jax.tree.map(lambda total, term: total + term.astype(jnp.float32), so_far, by_weights), by_h

    none_yet = {name: jnp.zeros(w.shape, jnp.float32) for name, w in weights.items()}
    by_weights, by_x = lax.scan(take, none_yet, (x, dy))
    return (by_x, *(by_weights[name].astype(jnp.bfloat16) for name in NAMES))
```

```python
import functools

import jax
import jax.numpy as jnp
from jax import lax
from jax.experimental import pallas as pl
from jax.experimental.pallas import tpu as pltpu
from jax.sharding import PartitionSpec as P

BF, F32 = jnp.bfloat16, jnp.float32
MESH = pl.DeviceIdType.MESH
ANY = pl.BlockSpec(memory_space=pl.ANY)
T, D, F, FP = 2048, 1280, 4480, 4608
SIDE, CORES = 4, 2
HALF = FP // 2
EPS = 1e-6
VMEM = 62 * 2**20
NT = (((1,), (1,)), ((), ()))
TN = (((0,), (0,)), ((), ()))


class Me:
    def __init__(self, places):
        s = lax.axis_index("s")
        self.places = places
        self.x = lax.axis_index("r")
        self.k = lax.rem(s, CORES)
        self.z = lax.rem(lax.div(s, CORES), SIDE)
        self.y = lax.div(s, CORES * SIDE)

    def at(self, dx=0, dy=0, dz=0, dk=0):
        y, z, k = lax.rem(self.y + dy, SIDE), lax.rem(self.z + dz, SIDE), lax.rem(self.k + dk, CORES)
        return {"r": lax.rem(self.x + dx, self.places), "s": (y * SIDE + z) * CORES + k}


class Task:
    ins, outs, scratch, copies, locals_ = (), (), (), 0, 0

    def events(self, steps):
        return {}


def copy(refs, number, src, dst, to):
    return pltpu.make_async_remote_copy(
        src_ref=src, dst_ref=dst, send_sem=refs.send.at[number], recv_sem=refs.recv.at[number], device_id=to, device_id_type=MESH
    )


class Refs:
    pass


class Gather(Task):
    PER_COLOUR = 15

    def __init__(self, kinds, blocks, slots):
        self.kinds, self.slots = kinds, slots
        self.ins = [(b, pl.BlockSpec(b.shape, lambda *_: (0, 0))) for b in blocks]
        self.outs = []
        for kind, b in zip(kinds, blocks):
            lead = (SIDE, SIDE, CORES) if kind == "row" else (SIDE, SIDE)
            self.outs.append(jax.ShapeDtypeStruct(lead + b.shape, b.dtype))
        self.copies = 2 * self.PER_COLOUR * len(kinds)
        self.locals_ = len(kinds)
        self.peers = {(0, 1, 0, 0), (0, 3, 0, 0), (0, 0, 1, 0), (0, 0, 3, 0), (0, 0, 0, 1)}

    def part(self, kind, ref, me, y, z, colour, half):
        if kind == "row":
            start, size = ((0, 2304), (2304, 2304))[colour] if half is None else (2304 * colour + 1152 * half, 1152)
            return ref.at[y, z, me.k, :, pl.ds(start, size)]
        if half is None:
            start, size = ((0, 144), (144, 136))[colour]
        else:
            start, size = (((0, 72), (72, 72)), ((144, 72), (216, 64)))[colour][half]
        return ref.at[y, z, pl.ds(start, size), pl.ds(pl.multiple_of(me.k * (D // 2), 128), D // 2)]

    def own(self, kind, ref, me, colour):
        if kind == "row":
            return ref.at[:, pl.ds(2304 * colour, 2304)]
        start, size = ((0, 144), (144, 136))[colour]
        return ref.at[pl.ds(start, size), pl.ds(pl.multiple_of(me.k * (D // 2), 128), D // 2)]

    def place(self, me, refs, n):
        whole = refs.outs[n]
        dst = whole.at[me.y, me.z, me.k] if self.kinds[n] == "row" else whole.at[me.y, me.z]
        return pltpu.make_async_copy(refs.ins[n], dst, refs.local.at[n])

    def region(self, me, refs, n, colour, phase, along, half=None):
        on_y = (colour == 0) == (phase == 0)
        every = slice(None)
        y = along if on_y else (every if phase else me.y)
        z = (every if phase else me.z) if on_y else along
        return self.part(self.kinds[n], refs.outs[n], me, y, z, colour, half)

    def ring(self, me, refs, n, colour, phase, hop, turn):
        on_y = (colour == 0) == (phase == 0)
        place = me.y if on_y else me.z
        base = (2 * n + colour) * self.PER_COLOUR + 4 * phase + 2 * hop + turn
        step = 1 if turn == 0 else SIDE - 1
        to = me.at(dy=step) if on_y else me.at(dz=step)
        from_ = place if hop == 0 else lax.rem(place + SIDE - step, SIDE)
        dst = self.region(me, refs, n, colour, phase, from_, None if hop == 0 else turn)
        src = dst
        if hop == 0 and phase == 0:
            src = self.own(self.kinds[n], refs.ins[n], me, colour)
        return copy(refs, base, src, dst, to)

    def across(self, me, refs, n, colour, phase, away):
        on_y = (colour == 0) == (phase == 0)
        place = lax.rem((me.y if on_y else me.z) + away, SIDE)
        ref = self.region(me, refs, n, colour, phase, place)
        return copy(refs, (2 * n + colour) * self.PER_COLOUR + 8 + 3 * phase + away - 1, ref, ref, me.at(dk=1))

    def over(self):
        return [(n, c) for n in range(len(self.kinds)) for c in range(2)]

    def events(self, steps):
        def start(me, refs):
            for n, c in self.over():
                for turn in range(2):
                    self.ring(me, refs, n, c, 0, 0, turn).start()
            for n in range(len(self.kinds)):
                self.place(me, refs, n).start()

        def forward(phase):
            def run(me, refs):
                for turn in range(2):
                    for n, c in self.over():
                        self.ring(me, refs, n, c, phase, 0, turn).wait_recv()
                        self.ring(me, refs, n, c, phase, 1, turn).start()
                for n, c in self.over():
                    for away in (1, 3):
                        self.across(me, refs, n, c, phase, away).start()

            return run

        def second(me, refs):
            for n in range(len(self.kinds)):
                self.place(me, refs, n).wait()
            for n in range(len(self.kinds)):
                if self.kinds[n] == "row":
                    self.both(me, refs, n).start()
            for n, c in self.over():
                for turn in range(2):
                    self.ring(me, refs, n, c, 0, 1, turn).wait_recv()
                for turn in range(2):
                    self.ring(me, refs, n, c, 1, 0, turn).start()
                self.across(me, refs, n, c, 0, 2).start()

        def last(me, refs):
            for n, c in self.over():
                for turn in range(2):
                    self.ring(me, refs, n, c, 1, 1, turn).wait_recv()
                self.across(me, refs, n, c, 1, 2).start()

        def end(me, refs):
            for n, c in self.over():
                for phase in range(2):
                    for hop in range(2):
                        for turn in range(2):
                            self.ring(me, refs, n, c, phase, hop, turn).wait_send()
                    for away in (1, 2, 3):
                        self.across(me, refs, n, c, phase, away).wait()
            for n in range(len(self.kinds)):
                if self.kinds[n] == "row":
                    self.both(me, refs, n).wait()

        made = [start, forward(0), second, forward(1), last]
        found = {}
        for slot, run in zip(self.slots, made):
            found.setdefault(min(slot, steps - 1), []).append(run)
        found["end"] = [end]
        return found

    def both(self, me, refs, n):
        ref = refs.outs[n].at[me.y, me.z, me.k]
        return copy(refs, 2 * n * self.PER_COLOUR + 14, refs.ins[n], ref, me.at(dk=1))


class Sends(Task):
    def __init__(self, arrays, outs, peers, plan, copies, local=None):
        self.ins = [(a, ANY) for a in arrays]
        self.outs, self.peers, self.plan, self.copies, self.local = outs, peers, plan, copies, local
        self.locals_ = 1 if local else 0

    def made(self, me, refs):
        return [copy(refs, i, *entry) for i, entry in enumerate(self.plan(me, refs.ins, refs.outs))]

    def events(self, steps):
        def start(me, refs):
            for c in self.made(me, refs):
                c.start()
            if self.local:
                pltpu.make_async_copy(*self.local(me, refs.ins, refs.outs), refs.local.at[0]).start()

        def end(me, refs):
            for c in self.made(me, refs):
                c.wait()
            if self.local:
                pltpu.make_async_copy(*self.local(me, refs.ins, refs.outs), refs.local.at[0]).wait()

        return {0: [start], "end": [end]}


def colours(kind, ref, lead, colour):
    if kind == "row":
        return ref.at[(*lead, slice(None), pl.ds(1152 * colour, 1152))]
    start, size = ((0, 144), (144, 136))[colour]
    return ref.at[(*lead, pl.ds(start, size), slice(None))]


def colour_shape(kind, colour):
    return (80, 1152) if kind == "row" else ((144, 136)[colour], D // 2)


def first_sends(kind, terms):
    shape = [jax.ShapeDtypeStruct((SIDE - 1, SIDE, *colour_shape(kind, c)), BF) for c in range(2)]

    def plan(me, ins, outs):
        found = []
        for d in (1, 3, 2):
            y, z = lax.rem(me.y + d, SIDE), lax.rem(me.z + d, SIDE)
            found.append((colours(kind, ins[0], (y, slice(None)), 0), outs[0].at[d - 1], me.at(dy=d)))
            found.append((colours(kind, ins[0], (slice(None), z), 1), outs[1].at[d - 1], me.at(dz=d)))
        return found

    peers = {(0, d, 0, 0) for d in (1, 2, 3)} | {(0, 0, d, 0) for d in (1, 2, 3)}
    return Sends([terms], shape, peers, plan, 6)


def second_sends(kind, along_y, along_z):
    shape = [jax.ShapeDtypeStruct((SIDE - 1, *colour_shape(kind, c)), BF) for c in range(2)]

    def plan(me, ins, outs):
        found = []
        for d in (1, 3, 2):
            y, z = lax.rem(me.y + d, SIDE), lax.rem(me.z + d, SIDE)
            found.append((ins[0].at[z], outs[0].at[d - 1], me.at(dz=d)))
            found.append((ins[1].at[y], outs[1].at[d - 1], me.at(dy=d)))
        return found

    peers = {(0, d, 0, 0) for d in (1, 2, 3)} | {(0, 0, d, 0) for d in (1, 2, 3)}
    return Sends([along_y, along_z], shape, peers, plan, 6)


def third_sends(kind, places, total):
    rows, columns = (40, HALF) if kind == "row" else (144, D // 2)
    shape = [jax.ShapeDtypeStruct((places, CORES, rows, columns), BF)]

    def window(me, ref, k):
        start = (40 if kind == "row" else 136) * k
        return ref.at[pl.ds(pl.multiple_of(start, 8), rows), :]

    def plan(me, ins, outs):
        found = []
        for dk in (0, 1):
            for dx in range(places):
                if (dx, dk) != (0, 0):
                    src = window(me, ins[0], lax.rem(me.k + dk, CORES))
                    found.append((src, outs[0].at[me.x, me.k], me.at(dx=dx, dk=dk)))
        return found

    def local(me, ins, outs):
        return window(me, ins[0], me.k), outs[0].at[me.x, me.k]

    peers = {(dx, 0, 0, dk) for dx in range(places) for dk in (0, 1)} - {(0, 0, 0, 0)}
    return Sends([total], shape, peers, plan, 2 * places - 1, local)


def fused(name, number, places, steps, compute, ins, outs, scratch=(), tasks=(), flops=0, extra_peers=(), partner=0):
    lists = [ins, *[t.ins for t in tasks]]
    n_in = [len(l) for l in lists]
    out_lists = [outs, *[[(o, ANY) for o in t.outs] for t in tasks]]
    n_out = [len(l) for l in out_lists]
    peers = sorted(set(extra_peers).union(*[t.peers for t in tasks]) if tasks else set(extra_peers))
    sems = []
    for t in tasks:
        sems += [pltpu.SemaphoreType.DMA((t.copies,)), pltpu.SemaphoreType.DMA((t.copies,)), pltpu.SemaphoreType.DMA((max(t.locals_, 1),))]
    if partner:
        sems += [pltpu.SemaphoreType.DMA((partner,)), pltpu.SemaphoreType.DMA((partner,))]

    def kernel(*refs):
        refs = list(refs)
        take = lambda n: [refs.pop(0) for _ in range(n)]
        given = [take(n) for n in n_in]
        made = [take(n) for n in n_out]
        own = take(len(scratch))
        held = []
        for i, t in enumerate(tasks):
            r = Refs()
            r.ins, r.outs = given[1 + i], made[1 + i]
            r.send, r.recv, r.local = take(3)
            held.append(r)
        pair = take(2) if partner else None
        me = Me(places)
        step = pl.program_id(0)

        if peers:

            @pl.when(step == 0)
            def _():
                barrier = pltpu.get_barrier_semaphore()
                for dx, dy, dz, dk in peers:
                    pl.semaphore_signal(barrier, inc=1, device_id=me.at(dx, dy, dz, dk), device_id_type=MESH)
                pl.semaphore_wait(barrier, len(peers))

        plans = [t.events(steps) for t in tasks]
        for slot in range(steps):
            runs = [(run, r) for plan, r in zip(plans, held) for run in plan.get(slot, ())]
            if runs:

                @pl.when(step == slot)
                def _():
                    for run, r in runs:
                        run(me, r)

        compute(step, me, given[0], made[0], own, pair)

        ends = [(run, r) for plan, r in zip(plans, held) for run in plan.get("end", ())]
        if ends:

            @pl.when(step == steps - 1)
            def _():
                for run, r in ends:
                    run(me, r)

    arrays = [a for l in lists for a, _ in l]
    got = pl.pallas_call(
        kernel,
        grid=(steps,),
        in_specs=[s for l in lists for _, s in l],
        out_specs=[s for l in out_lists for _, s in l],
        out_shape=[o for l in out_lists for o, _ in l],
        scratch_shapes=[*scratch, *sems],
        name=name,
        cost_estimate=pl.CostEstimate(flops=int(flops), bytes_accessed=1 << 24, transcendentals=0),
        compiler_params=pltpu.CompilerParams(
            vmem_limit_bytes=VMEM,
            has_side_effects=bool(peers),
            **({"collective_id": number} if peers else {}),
        ),
    )(*arrays)
    got = list(got)
    return [[got.pop(0) for _ in range(n)] for n in n_out]


def whole(shape):
    return pl.BlockSpec(shape, lambda j: (0,) * len(shape))


def shaped(*shape, dtype=BF):
    return jax.ShapeDtypeStruct(shape, dtype)


def sigmoid(g):
    return 1.0 / (1.0 + jnp.exp(-g))


def chunks(total, size, body):
    size = min(size, total)

    def run(i, _):
        body(pl.ds(pl.multiple_of(i * size, size), size))
        return 0

    lax.fori_loop(0, total // size, run, 0)


def scale_of(wide):
    return lax.rsqrt(jnp.mean(wide * wide, -1, keepdims=True) + EPS)


def norm_kernel(number, places, x, tasks):
    steps = 8
    rows = T // steps

    def compute(step, me, ins, outs, own, pair):
        def body(r):
            wide = ins[0][r, :].astype(F32)
            outs[0][r, :] = (wide * scale_of(wide)).astype(BF)

        chunks(rows, 64, body)

    block = pl.BlockSpec((rows, D), lambda j: (j, 0))
    return fused("norm", number, places, steps, compute, [(x, block)], [(shaped(T, D), block)], tasks=tasks, flops=10 * T * D)


def gate_up_kernel(number, places, a, wg, wu, tasks, bn=512, mc=1024):
    def compute(step, me, ins, outs, own, pair):
        a, wg, wu = ins
        g_o, u_o, act_o = outs

        def body(r):
            rows = a[r, :]
            g = jnp.dot(rows, wg[...], preferred_element_type=F32)
            u = jnp.dot(rows, wu[...], preferred_element_type=F32)
            g_o[r, :] = g
            u_o[r, :] = u
            act_o[r, :] = (g * sigmoid(g) * u).astype(BF)

        chunks(T, mc, body)

    block = pl.BlockSpec((T, bn), lambda j: (0, j))
    w = pl.BlockSpec((D, bn), lambda j: (0, j))
    return fused(
        "gate_up", number, places, FP // bn, compute, [(a, whole((T, D))), (wg, w), (wu, w)],
        [(shaped(T, FP, dtype=F32), block), (shaped(T, FP, dtype=F32), block), (shaped(T, FP), block)], tasks=tasks, flops=4 * T * D * FP,
    )


def down_kernel(number, places, act, wd, h, tasks, bk=512, mc=512):
    steps = FP // bk
    tail = F - (steps - 1) * bk

    def compute(step, me, ins, outs, own, pair):
        act, wd, h = ins
        h_o, a_o = outs
        (acc,) = own

        @pl.when(step == 0)
        def _():
            def zero(r):
                acc[r, :] = jnp.zeros((min(128, acc.shape[0]), D), F32)

            chunks(T, 128, zero)

        def add(depth):
            def body(r):
                acc[r, :] = acc[r, :] + jnp.dot(act[r, :depth], wd[:depth, :], preferred_element_type=F32)

            chunks(T, mc, body)

        @pl.when(step < steps - 1)
        def _():
            add(bk)

        @pl.when(step == steps - 1)
        def _():
            add(tail)

            def finish(r):
                y = (h[r, :].astype(F32) + acc[r, :].astype(BF).astype(F32)).astype(BF)
                h_o[r, :] = y
                wide = y.astype(F32)
                a_o[r, :] = (wide * scale_of(wide)).astype(BF)

            chunks(T, 64, finish)

    return fused(
        "down", number, places, steps, compute,
        [(act, pl.BlockSpec((T, bk), lambda j: (0, j))), (wd, pl.BlockSpec((bk, D), lambda j: (j, 0))), (h, whole((T, D)))],
        [(shaped(T, D), whole((T, D))), (shaped(T, D), whole((T, D)))], [pltpu.VMEM((T, D), F32)], tasks=tasks, flops=2 * T * D * FP,
    )


def by_act_kernel(number, places, by_h, wd, g, u, tasks, bn=512, mc=512):
    def compute(step, me, ins, outs, own, pair):
        by_h, wd, g, u = ins
        dg_o, du_o = outs
        inside = lax.broadcasted_iota(jnp.int32, (min(mc, T), bn), 1) + step * bn < F

        def body(r):
            d = lax.dot_general(by_h[r, :], wd[...], NT, preferred_element_type=F32)
            d = jnp.where(inside, d, 0.0).astype(BF).astype(F32)
            gate, up = g[r, :], u[r, :]
            s = sigmoid(gate)
            gs = gate * s
            du_o[r, :] = (d * gs).astype(BF)
            dg_o[r, :] = (d * up * (s + gs * (1.0 - s))).astype(BF)

        chunks(T, mc, body)

    block = pl.BlockSpec((T, bn), lambda j: (0, j))
    return fused(
        "by_act", number, places, FP // bn, compute,
        [(by_h, whole((T, D))), (wd, pl.BlockSpec((bn, D), lambda j: (j, 0))), (g, block), (u, block)],
        [(shaped(T, FP), block), (shaped(T, FP), block)], tasks=tasks, flops=2 * T * D * FP,
    )


def by_row_kernel(number, places, a, dg, tasks, bn=768, mc=640):
    n = HALF // bn

    def columns(j):
        k = lax.rem(lax.axis_index("s"), CORES)
        return (0, jnp.where(j < n, (1 - k) * n + j, k * n + j - n))

    def compute(step, me, ins, outs, own, pair):
        a, dg = ins
        sum_o, wide_o = outs
        mine, theirs = own

        def send(i):
            return pltpu.make_async_remote_copy(
                src_ref=mine.at[i], dst_ref=theirs.at[i], send_sem=pair[0].at[i], recv_sem=pair[1].at[i], device_id=me.at(dk=1), device_id_type=MESH
            )

        def dot(r):
            return lax.dot_general(a[:, r], dg[...], TN, preferred_element_type=F32)

        for i in range(n):

            @pl.when(step == i + 1)
            def _():
                send(i).start()

        @pl.when(step < n)
        def _():
            def body(r):
                mine[step, r, :] = dot(r).astype(BF)

            chunks(D, mc, body)

        for i in range(n):

            @pl.when(step == n + i)
            def _():
                send(i).wait_recv()

        @pl.when(step >= n)
        def _():
            def body(r):
                total = dot(r) + theirs[step - n, r, :].astype(F32)
                wide_o[r, :] = total
                sum_o[r, :] = total.astype(BF)

            chunks(D, mc, body)

        @pl.when(step == 2 * n - 1)
        def _():
            for i in range(n):
                send(i).wait_send()

    out = pl.BlockSpec((D, bn), lambda j: (0, jnp.maximum(j - n, 0)))
    return fused(
        "by_row", number, places, 2 * n, compute, [(a, whole((T, D))), (dg, pl.BlockSpec((T, bn), columns))],
        [(shaped(D, HALF), out), (shaped(D, HALF, dtype=F32), out)],
        [pltpu.VMEM((n, D, bn), BF), pltpu.VMEM((n, D, bn), BF)], tasks=tasks, flops=2 * T * D * FP, extra_peers={(0, 0, 0, 1)}, partner=n,
    )


def by_down_kernel(number, places, act, by_h, tasks, bm=768, mc=384):
    n = FP // bm
    width = D // 2

    def compute(step, me, ins, outs, own, pair):
        act, by_h = ins
        sum_o, wide_o = outs
        mine, theirs = own
        half = jnp.where(step < n, 1 - me.k, me.k)
        columns = pl.ds(pl.multiple_of(half * width, 128), width)

        def send(i):
            return pltpu.make_async_remote_copy(
                src_ref=mine.at[i], dst_ref=theirs.at[i], send_sem=pair[0].at[i], recv_sem=pair[1].at[i], device_id=me.at(dk=1), device_id_type=MESH
            )

        def dot(r):
            return lax.dot_general(act[:, r], by_h[:, columns], TN, preferred_element_type=F32)

        for i in range(n):

            @pl.when(step == i + 1)
            def _():
                send(i).start()

        @pl.when(step < n)
        def _():
            def body(r):
                mine[step, r, :] = dot(r).astype(BF)

            chunks(bm, mc, body)

        for i in range(n):

            @pl.when(step == n + i)
            def _():
                send(i).wait_recv()

        @pl.when(step >= n)
        def _():
            def body(r):
                total = dot(r) + theirs[step - n, r, :].astype(F32)
                wide_o[r, :] = total
                sum_o[r, :] = total.astype(BF)

            chunks(bm, mc, body)

        @pl.when(step == 2 * n - 1)
        def _():
            for i in range(n):
                send(i).wait_send()

    out = pl.BlockSpec((bm, width), lambda j: (jnp.maximum(j - n, 0), 0))
    return fused(
        "by_down", number, places, 2 * n, compute,
        [(act, pl.BlockSpec((T, bm), lambda j: (0, lax.rem(j, n)))), (by_h, whole((T, D)))],
        [(shaped(F, width), out), (shaped(F, width, dtype=F32), out)],
        [pltpu.VMEM((n, bm, width), BF), pltpu.VMEM((n, bm, width), BF)], tasks=tasks, flops=2 * T * D * FP, extra_peers={(0, 0, 0, 1)}, partner=n,
    )


def by_input_kernel(number, places, dg, du, wg, wu, h, by_h, tasks, part=0, parts=1, bk=512, mc=1024):
    steps = FP // bk
    rows = T // parts

    def compute(step, me, ins, outs, own, pair):
        dg, du, wg, wu, h, by_h = ins
        (acc,) = own

        @pl.when(step == 0)
        def _():
            def zero(r):
                acc[r, :] = jnp.zeros((min(128, acc.shape[0]), D), F32)

            chunks(rows, 128, zero)

        def body(r):
            p = lax.dot_general(dg[r, :], wg[...], NT, preferred_element_type=F32)
            p = p + lax.dot_general(du[r, :], wu[...], NT, preferred_element_type=F32)
            acc[r, :] = acc[r, :] + p

        chunks(rows, mc, body)

        @pl.when(step == steps - 1)
        def _():
            def finish(r):
                by_a = acc[r, :].astype(BF).astype(F32)
                wide = h[r, :].astype(F32)
                scale = scale_of(wide)
                along = jnp.sum(by_a * wide, -1, keepdims=True)
                by_wide = by_a * scale - wide * (scale * scale * scale * along * (1.0 / D))
                outs[0][r, :] = (by_h[r, :].astype(F32) + by_wide.astype(BF).astype(F32)).astype(BF)

            chunks(rows, 64, finish)

    tokens = pl.BlockSpec((rows, bk), lambda j: (part, j))
    w = pl.BlockSpec((D, bk), lambda j: (0, j))
    block = pl.BlockSpec((rows, D), lambda j: (part, 0))
    return fused(
        "by_input", number, places, steps, compute,
        [(dg, tokens), (du, tokens), (wg, w), (wu, w), (h, block), (by_h, block)],
        [(shaped(rows, D), whole((rows, D)))], [pltpu.VMEM((rows, D), F32)], tasks=tasks, flops=4 * rows * D * FP,
    )


def sends_kernel(number, places, tasks):
    def compute(step, me, ins, outs, own, pair):
        pass

    return fused("sends", number, places, 1, compute, [], [], tasks=tasks)


class Sum:
    def __init__(self, kind, me, places, made):
        self.kind, self.me, self.places = kind, me, places
        self.narrow, self.wide = (m.reshape(SIDE, SIDE, m.shape[0] // SIDE**2, m.shape[1]) for m in made)

    def first(self):
        return first_sends(self.kind, self.narrow)

    def after_first(self, got):
        y, z, _, _ = self.me
        c = lambda n: (slice(None), slice(None), slice(1152 * n, 1152 * n + 1152)) if self.kind == "row" else (slice(None), slice(*((0, 144), (144, 280))[n]))
        own_y = lax.dynamic_index_in_dim(self.wide, y, 0, keepdims=False)[c(0)]
        own_z = lax.dynamic_index_in_dim(self.wide, z, 1, keepdims=False)[c(1)]
        self.sums = [own + got[n][0].astype(F32) + got[n][1].astype(F32) + got[n][2].astype(F32) for n, own in enumerate((own_y, own_z))]
        self.narrow = [s.astype(BF) for s in self.sums]

    def second(self):
        return second_sends(self.kind, *self.narrow)

    def after_second(self, got):
        y, z, _, _ = self.me
        own = [lax.dynamic_index_in_dim(s, i, 0, keepdims=False) for s, i in zip(self.sums, (z, y))]
        sums = [o + g[0].astype(F32) + g[1].astype(F32) + g[2].astype(F32) for o, g in zip(own, got)]
        self.total = jnp.concatenate(sums, 1 if self.kind == "row" else 0).astype(BF)

    def third(self):
        return third_sends(self.kind, self.places, self.total)

    def done(self, got):
        terms = got[0].astype(F32)
        total = terms[0]
        for i in range(1, self.places):
            total = total + terms[i]
        if self.kind == "row":
            return jnp.concatenate([total[0], total[1]], 1)[:, :F].astype(BF)
        k = self.me[2]
        rows = F // SIDE**2 // CORES
        both = jnp.concatenate([total[0], total[1]], 1)
        return jnp.where(k == 0, both[:rows], both[144 - rows :]).astype(BF)


def solution(mesh):
    places = mesh.shape["r"]

    def step(x, dy, w_gate, w_up, w_down):
        x, dy = x[0], dy[0]
        s = lax.axis_index("s")
        k = s % CORES
        me = (s // (CORES * SIDE), (s // CORES) % SIDE, k, lax.axis_index("r"))
        n_s = SIDE * SIDE * CORES
        gate = [jnp.pad(w_gate[i], ((0, 0), (0, FP - F))) for i in range(2)]
        up = [jnp.pad(w_up[i], ((0, 0), (0, FP - F))) for i in range(2)]
        other = lax.ppermute(w_down, "s", [(i, i ^ 1) for i in range(n_s)])
        down = jnp.where(k == 0, jnp.concatenate([w_down, other], 1), jnp.concatenate([other, w_down], 1))
        rows = lambda m: m.reshape(D, FP)
        chip = lambda m: m.reshape(F, D)
        add = functools.partial(Sum, me=me, places=places)

        (a0,), (g0, u0) = norm_kernel(0, places, x, [Gather(["row", "row"], [gate[0], up[0]], (0, 1, 2, 4, 6))])
        wg0, wu0 = rows(g0), rows(u0)
        (gate0, up0, act0), (d0, g1) = gate_up_kernel(1, places, a0, wg0, wu0, [Gather(["chip", "row"], [down[0], gate[1]], (0, 1, 2, 6, 8))])
        wd0, wg1 = chip(d0), rows(g1)
        (h1, a1), (u1,) = down_kernel(2, places, act0, wd0, x, [Gather(["row"], [up[1]], (0, 1, 2, 6, 8))])
        wu1 = rows(u1)
        (gate1, up1, act1), (d1,) = gate_up_kernel(3, places, a1, wg1, wu1, [Gather(["chip"], [down[1]], (0, 1, 2, 5, 7))])
        wd1 = chip(d1)

        ((dg1, du1),) = by_act_kernel(4, places, dy, wd1, gate1, up1, [])
        (made,) = by_down_kernel(5, places, act1, dy, [])
        sum_d1 = add("chip", made=made)
        made, got = by_row_kernel(6, places, a1, dg1, [sum_d1.first()])
        sum_d1.after_first(got)
        sum_g1 = add("row", made=made)
        (by_h1,), got, more = by_input_kernel(7, places, dg1, du1, wg1, wu1, h1, dy, [sum_g1.first(), sum_d1.second()])
        sum_g1.after_first(got)
        sum_d1.after_second(more)
        made, got, more = by_down_kernel(8, places, act0, by_h1, [sum_d1.third(), sum_g1.second()])
        out_d1 = sum_d1.done(got)
        sum_g1.after_second(more)
        sum_d0 = add("chip", made=made)
        made, got = by_row_kernel(9, places, a1, du1, [sum_d0.first()])
        sum_d0.after_first(got)
        sum_u1 = add("row", made=made)
        (dg0, du0), got, more, last = by_act_kernel(10, places, by_h1, wd0, gate0, up0, [sum_u1.first(), sum_g1.third(), sum_d0.second()])
        sum_u1.after_first(got)
        out_g1 = sum_g1.done(more)
        sum_d0.after_second(last)
        made, got, more = by_row_kernel(11, places, a0, dg0, [sum_u1.second(), sum_d0.third()])
        sum_u1.after_second(got)
        out_d0 = sum_d0.done(more)
        sum_g0 = add("row", made=made)
        made, got, more = by_row_kernel(12, places, a0, du0, [sum_g0.first(), sum_u1.third()])
        sum_g0.after_first(got)
        out_u1 = sum_u1.done(more)
        sum_u0 = add("row", made=made)
        (low,), got, more = by_input_kernel(13, places, dg0, du0, wg0, wu0, x, by_h1, [sum_u0.first(), sum_g0.second()], 0, 2)
        sum_u0.after_first(got)
        sum_g0.after_second(more)
        (high,), got, more = by_input_kernel(14, places, dg0, du0, wg0, wu0, x, by_h1, [sum_u0.second(), sum_g0.third()], 1, 2)
        sum_u0.after_second(got)
        out_g0 = sum_g0.done(more)
        _, got = sends_kernel(15, places, [sum_u0.third()])
        out_u0 = sum_u0.done(got)
        by_x = jnp.concatenate([low, high], 0)
        return by_x[None], jnp.stack([out_g0, out_g1]), jnp.stack([out_u0, out_u1]), jnp.stack([out_d0, out_d1])

    states, cut = P(("rep", "r", "s"), None, None), P(None, "s", None)
    return jax.shard_map(
        step,
        mesh=mesh,
        in_specs=(states, states) + (cut,) * 3,
        out_specs=(states,) + (P("rep", "s", None),) * 3,
        check_vma=False,
    )
```
